32 devices in a mesh: fsdp: 2 (over x), ctx: 4 (over z), tp: 4 (over y, core).
Axes of the slice: x: 2, y: 2, z: 4, core: 2. Of those that a mesh axis runs over, the one named last changes fastest.
Arguments:
- tokens: bfloat16 [2, 8192, 768], P(None, ('fsdp', 'ctx')), may hold values from -6 to 6
- encoder_states: bfloat16 [2, 8192, 768], P(None, ('fsdp', 'ctx')), may hold values from -6 to 6
- lengths: int32 [2, 2, 2], P(None, 'fsdp'), may hold values from 1 to 3072, 4096 in all within a row
- enc_pick: int32 [2, 16, 1024], P(None, ('fsdp', 'ctx')), may hold values from 0 to 2047, as said below
- cotangent: bfloat16 [2, 8192, 768], P(None, ('fsdp', 'ctx', 'tp')), may hold values from -6 to 6
- w_self: bfloat16 [768, 3, 768], P('fsdp', None, 'tp'), may hold values from -0.21875 to 0.21875
- w_self_out: bfloat16 [768, 768], P('fsdp', 'tp'), may hold values from -0.875 to 0.875
- w_cross: bfloat16 [768, 3, 768], P('fsdp', None, 'tp'), may hold values from -0.21875 to 0.21875
- w_cross_out: bfloat16 [768, 768], P('fsdp', 'tp'), may hold values from -0.875 to 0.875
- w_up: bfloat16 [768, 3072], P('fsdp', 'tp'), may hold values from -0.21875 to 0.21875
- w_down: bfloat16 [768, 3072], P('fsdp', 'tp'), may hold values from -0.109375 to 0.109375
- b_self: bfloat16 [2, 768], P(None, 'tp'), may hold values from -3 to 3
- b_cross: bfloat16 [2, 768], P(None, 'tp'), may hold values from -3 to 3
- b_up: bfloat16 [3072], P('tp'), may hold values from -3 to 3
- out_bias: bfloat16 [3, 768], replicated, may hold values from -3 to 3
- ln_gain: bfloat16 [3, 768], replicated, may hold values from 0.5 to 1.5
- ln_shift: bfloat16 [3, 768], replicated, may hold values from -3 to 3
Outputs:
- layer_out: float32 [2, 8192, 768], P(None, ('fsdp', 'ctx', 'tp'))
- grad_tokens: float32 [2, 8192, 768], P(None, ('fsdp', 'ctx', 'tp'))
- grad_encoder: float32 [2, 8192, 768], P(None, ('fsdp', 'ctx', 'tp'))
- grad_w_self: float32 [768, 3, 768], P('fsdp', None, 'tp')
- grad_w_self_out: float32 [768, 768], P('fsdp', 'tp')
- grad_w_cross: float32 [768, 3, 768], P('fsdp', None, 'tp')
- grad_w_cross_out: float32 [768, 768], P('fsdp', 'tp')
- grad_w_up: float32 [768, 3072], P('fsdp', 'tp')
- grad_w_down: float32 [768, 3072], P('fsdp', 'tp')
- grad_b_self: float32 [2, 768], P(None, 'tp')
- grad_b_cross: float32 [2, 768], P(None, 'tp')
- grad_b_up: float32 [3072], P('tp')
- grad_out_bias: float32 [3, 768], replicated
- grad_ln_gain: float32 [3, 768], replicated
- grad_ln_shift: float32 [3, 768], replicated
The draws below stay inside these ranges and needn't reach their ends.
Inputs may be any that keep to these rules, and one draw needn't show every extreme that they name: The two lengths of a token group sum to 4096; the first lies from 1024 to 3072, the second is 4096 minus it. `enc_pick`: the 1024 positions of a row are distinct.
All inputs are finite; a program needn't handle non-finite values.
Results may differ from the reference program's by a relative error of at most 0.025.
Values may be sent and summed in bfloat16 or wider, within the bound.
A program may use at most 384 MiB of HBM per device.

```python
import math
import jax
import jax.numpy as jnp
import numpy as np
from jax import lax

D = 768
HEAD = 64
FF = 3072
MICRO = 2
QBLK = 512
TOPK = 1024
ENC_LEN = 2048
GROUP = 4096
TOKENS = 8192
ENCODER = 8192
QBLOCKS = 16
N_FSDP = 2


def draw_enc_pick(key, part):
    row_keys = jax.random.split(key, MICRO * QBLOCKS)

    def one_row(row_key):
        chosen = jax.random.permutation(row_key, ENC_LEN)[:TOPK]
        has_last = jnp.any(chosen == ENC_LEN - 1)
        return chosen.at[0].set(jnp.where(has_last, chosen[0], ENC_LEN - 1))
    picked = jax.vmap(one_row)(row_keys)
    return picked.reshape(MICRO, QBLOCKS, TOPK).astype(jnp.int32)


def steps_of(rng, shape, pieces, least, top_value):
    def one(axis_at, blocks):
        steps = jax.random.uniform(jax.random.fold_in(jax.random.fold_in(rng, 6), axis_at), (blocks,), jnp.float32, least / len(pieces), top_value / len(pieces))
        return jnp.repeat(jnp.exp(steps), shape[axis_at] // blocks).reshape((-1,) + (1,) * (len(shape) - axis_at - 1))

    level = one(*pieces[0])
    for cut in pieces[1:]:
        level = level * one(*cut)
    return level


def split_up(number_of, total, most, slope):
    loads = [(1 << 20) // math.isqrt(grade ** slope) + 1 for grade in range(2, number_of + 1)]
    rest, holding = total - most - (number_of - 1), [1] * (number_of - 1)
    while rest > 0:
        free = [i for i in range(number_of - 1) if holding[i] < most]
        whole, left = sum([loads[i] for i in free]), rest
        for i in free:
            more = min(most - holding[i], max(1, left * loads[i] // whole), rest)
            holding[i] = holding[i] + more
            rest = rest - more
    return np.array([most] + holding)


def ragged_sizes(own_key, number_of, total, most, slope):
    if number_of == 2:
        one = jax.random.randint(own_key, (), max(1, total - most), min(most, total - 1) + 1)
        return jnp.stack([one, total - one])
    sizes = jnp.asarray(split_up(number_of, total, most, slope), jnp.int32)
    couples = (number_of - 1) // 2
    source_of, receiver = sizes[1:1 + 2 * couples:2], sizes[2:2 + 2 * couples:2]
    slack = jnp.minimum(source_of - 1, most - receiver)
    moved = jax.random.randint(jax.random.fold_in(own_key, 1), (couples,), 0, 1 << 20) % (slack + 1)
    sizes = sizes.at[1:1 + 2 * couples:2].set(source_of - moved).at[2:2 + 2 * couples:2].set(receiver + moved)
    return sizes[jax.random.permutation(jax.random.fold_in(own_key, 2), number_of)]


def scatter_about(rng, shape, scale, limit, shards=(), held_as=jnp.bfloat16):
    drawn = scale * jax.random.normal(rng, shape, jnp.float32)
    if shards:
        drawn = drawn * steps_of(rng, shape, shards, -0.22, 0.18)
    return jnp.clip(drawn, -limit, limit).astype(held_as)


def setup_inputs(seed: int = 0) -> dict:
    arg_keys = jax.random.split(jax.random.key(seed), 18)
    tokens = scatter_about(arg_keys[0], (MICRO, TOKENS, D), 1.0, 6.0, ((1, 8),))
    encoder_states = scatter_about(arg_keys[1], (MICRO, ENCODER, D), 1.0, 6.0, ((1, 8),))
    lengths = jax.vmap(lambda own: ragged_sizes(own, 2, GROUP, GROUP * 3 // 4, 0))(jax.random.split(arg_keys[2], MICRO * N_FSDP)).reshape((MICRO, N_FSDP, 2)).astype(jnp.int32)
    enc_pick = draw_enc_pick(jax.random.fold_in(arg_keys[17], 71), 0)
    cotangent = scatter_about(arg_keys[4], (MICRO, TOKENS, D), 1.0, 6.0, ((1, 32),))
    w_self = scatter_about(arg_keys[5], (D, 3, D), D ** -0.5, 0.21875, ((0, 2), (2, 4)))
    w_self_out = scatter_about(arg_keys[6], (D, D), (D // 16) ** -0.5, 0.875, ((0, 2), (1, 4)))
    w_cross = scatter_about(arg_keys[7], (D, 3, D), D ** -0.5, 0.21875, ((0, 2), (2, 4)))
    w_cross_out = scatter_about(arg_keys[8], (D, D), (D // 16) ** -0.5, 0.875, ((0, 2), (1, 4)))
    w_up = scatter_about(arg_keys[9], (D, FF), D ** -0.5, 0.21875, ((0, 2), (1, 4)))
    w_down = scatter_about(arg_keys[10], (D, FF), FF ** -0.5, 0.109375, ((0, 2), (1, 4)))
    b_self = scatter_about(arg_keys[11], (2, D), 0.3, 3.0, ((1, 4),))
    b_cross = scatter_about(arg_keys[12], (2, D), 0.3, 3.0, ((1, 4),))
    b_up = scatter_about(arg_keys[13], (FF,), 0.3, 3.0, ((0, 4),))
    out_bias = scatter_about(arg_keys[14], (3, D), 0.3, 3.0)
    ln_gain = jnp.clip(1.0 + 0.1 * jax.random.normal(arg_keys[15], (3, D), jnp.float32), 0.5, 1.5).astype(jnp.bfloat16)
    ln_shift = scatter_about(arg_keys[16], (3, D), 0.3, 3.0)
    return dict(tokens=tokens, encoder_states=encoder_states, lengths=lengths, enc_pick=enc_pick, cotangent=cotangent, w_self=w_self, w_self_out=w_self_out, w_cross=w_cross, w_cross_out=w_cross_out, w_up=w_up, w_down=w_down, b_self=b_self, b_cross=b_cross, b_up=b_up, out_bias=out_bias, ln_gain=ln_gain, ln_shift=ln_shift)


@jax.custom_vjp
def low(v):
    return lax.optimization_barrier(v.astype(jnp.bfloat16)).astype(jnp.float32)

@jax.custom_vjp
def low_back(v):
    return v

def low_keep(v):
    return (low(v), None)

def low_pass(kept, grad):
    return (grad,)

def back_keep(v):
    return (v, None)

def back_low(kept, grad):
    return (low(grad),)
low.defvjp(low_keep, low_pass)
low_back.defvjp(back_keep, back_low)

def layer_norm(residual, norm_gain, norm_shift):
    average = lax.optimization_barrier(jnp.mean(residual, axis=-1, keepdims=True))
    centred = residual - average
    variance = lax.optimization_barrier(jnp.mean(centred * centred, axis=-1, keepdims=True))
    return centred * lax.rsqrt(variance + 1e-05) * norm_gain + norm_shift

def rounded_both(operand):
    return low_back(low(operand))

def matmul_high(left, right):
    return jnp.dot(left, right, precision=lax.Precision.HIGHEST)

def softmax_rows(scores):
    largest = lax.optimization_barrier(jnp.max(scores, axis=-1, keepdims=True))
    exponent = jnp.exp(scores - largest)
    return exponent / lax.optimization_barrier(jnp.sum(exponent, axis=-1, keepdims=True))

def pack_forward(params, token_rows, enc_rows, first_len, pick_rows):
    w_self, w_self_out, w_cross, w_cross_out, w_up, w_down, b_self, b_cross, b_up, out_bias, ln_gain, ln_shift = params
    group_len = token_rows.shape[0]
    head_count = D // HEAD
    scaling = HEAD ** (-0.5)
    positions = jnp.arange(group_len, dtype=jnp.int32)
    segment = (positions >= first_len).astype(jnp.int32)
    queries = rounded_both(matmul_high(token_rows, w_self[:, 0]) + b_self[0])
    keys_all = rounded_both(matmul_high(token_rows, w_self[:, 1]))
    values_all = rounded_both(matmul_high(token_rows, w_self[:, 2]) + b_self[1])
    key_heads = keys_all.reshape(group_len, head_count, HEAD)
    value_heads = values_all.reshape(group_len, head_count, HEAD)
    block_count = group_len // QBLK

    def self_block(block_args):
        query_block, place_block, seg_block = block_args
        scores = jnp.einsum('qhe,khe->hqk', query_block.reshape(QBLK, head_count, HEAD), key_heads, precision=lax.Precision.HIGHEST) * scaling
        scores = low_back(scores)
        allowed = (positions[None, :] <= place_block[:, None]) & (segment[None, :] == seg_block[:, None])
        scores = jnp.where(allowed[None], scores, -1e+30)
        attn_prob = low(softmax_rows(scores))
        return jnp.einsum('hqk,khe->qhe', attn_prob, value_heads, precision=lax.Precision.HIGHEST).reshape(QBLK, D)
    attended = lax.map(jax.checkpoint(self_block), (queries.reshape(block_count, QBLK, D), positions.reshape(block_count, QBLK), segment.reshape(block_count, QBLK)))
    attended = rounded_both(attended.reshape(group_len, D))
    branch = low_back(matmul_high(attended, w_self_out.T)) + out_bias[0]
    first_out = low(layer_norm(token_rows + branch, ln_gain[0], ln_shift[0]))
    cross_query = rounded_both(matmul_high(first_out, w_cross[:, 0]) + b_cross[0])
    enc_keys = rounded_both(matmul_high(enc_rows, w_cross[:, 1]))
    enc_values = rounded_both(matmul_high(enc_rows, w_cross[:, 2]) + b_cross[1])
    enc_length = enc_rows.shape[0] // 2
    block_start = jnp.arange(block_count, dtype=jnp.int32) * QBLK
    picked = pick_rows + (block_start >= first_len).astype(jnp.int32)[:, None] * enc_length

    def cross_block(block_args):
        query_block, picked_rows = block_args
        picked_keys = enc_keys[picked_rows].reshape(TOPK, head_count, HEAD)
        picked_values = enc_values[picked_rows].reshape(TOPK, head_count, HEAD)
        scores = jnp.einsum('qhe,khe->hqk', query_block.reshape(QBLK, head_count, HEAD), picked_keys, precision=lax.Precision.HIGHEST) * scaling
        scores = low_back(scores)
        attn_prob = low(softmax_rows(scores))
        return jnp.einsum('hqk,khe->qhe', attn_prob, picked_values, precision=lax.Precision.HIGHEST).reshape(QBLK, D)
    cross_att = lax.map(jax.checkpoint(cross_block), (cross_query.reshape(block_count, QBLK, D), picked))
    cross_att = rounded_both(cross_att.reshape(group_len, D))
    cross_branch = low_back(matmul_high(cross_att, w_cross_out.T)) + out_bias[1]
    second_out = low(layer_norm(first_out + cross_branch, ln_gain[1], ln_shift[1]))
    hidden = low_back(matmul_high(second_out, w_up) + b_up)
    activation = low(jax.nn.gelu(hidden, approximate=False))
    ffn_branch = low_back(matmul_high(activation, w_down.T)) + out_bias[2]
    return layer_norm(second_out + ffn_branch, ln_gain[2], ln_shift[2])

def reference(tokens, encoder_states, lengths, enc_pick, cotangent, w_self, w_self_out, w_cross, w_cross_out, w_up, w_down, b_self, b_cross, b_up, out_bias, ln_gain, ln_shift):
    packs = MICRO * N_FSDP
    params = tuple((item.astype(jnp.float32) for item in (w_self, w_self_out, w_cross, w_cross_out, w_up, w_down, b_self, b_cross, b_up, out_bias, ln_gain, ln_shift)))
    inputs = (tokens.astype(jnp.float32).reshape(packs, GROUP, D), encoder_states.astype(jnp.float32).reshape(packs, 2 * ENC_LEN, D), lengths[:, :, 0].reshape(packs), enc_pick.reshape(packs, GROUP // QBLK, TOPK), cotangent.astype(jnp.float32).reshape(packs, GROUP, D))

    def pack_step(running, pack_item):
        token_rows, enc_rows, first_len, pick_rows, upstream = pack_item
        pack_out, pullback = jax.vjp(lambda param_set, left_rows, right_rows: pack_forward(param_set, left_rows, right_rows, first_len, pick_rows), params, token_rows, enc_rows)
        grad_params, grad_rows, grad_enc = pullback(upstream)
        return (jax.tree.map(jnp.add, running, grad_params), (pack_out, grad_rows, grad_enc))
    initial = jax.tree.map(jnp.zeros_like, params)
    totals, (pack_outs, grad_rows, grad_enc) = lax.scan(pack_step, initial, inputs)
    return (pack_outs.reshape(MICRO, TOKENS, D), grad_rows.reshape(MICRO, TOKENS, D), grad_enc.reshape(MICRO, ENCODER, D), totals[0], totals[1], totals[2], totals[3], totals[4], totals[5], totals[6], totals[7], totals[8], totals[9], totals[10], totals[11])
```

```python
import functools

import jax
import jax.numpy as jnp
from jax import lax
from jax.experimental import pallas as pl
from jax.experimental.pallas import tpu as pltpu
from jax.sharding import PartitionSpec as P

HEAD = 64
LANES = 128
QBLK = 512
TILE = 256
NEG_FILL = -1e30
SCALING = HEAD ** (-0.5)


BF = jnp.bfloat16
F32 = jnp.float32


def nt(left, right):
    return lax.dot_general(
        left, right, (((1,), (1,)), ((), ())), preferred_element_type=F32
    )


def nn(left, right):
    return lax.dot_general(
        left, right, (((1,), (0,)), ((), ())), preferred_element_type=F32
    )


def tn(left, right):
    return lax.dot_general(
        left, right, (((0,), (0,)), ((), ())), preferred_element_type=F32
    )


def chunk_state(info, qi, back, chunk_len):
    first_len = info[8]
    chunk = info[9] - back
    q_start = info[qi]
    starts_second = q_start >= first_len
    touches_second = q_start + TILE > first_len
    whole_first = (chunk + 1) * chunk_len <= first_len
    part_first = chunk * chunk_len < first_len
    active = (chunk >= 0) & jnp.logical_not(starts_second & whole_first)
    masked = touches_second & part_first
    return active, masked, chunk


def self_mask(info, qi, chunk, chunk_len, kp_ref):
    first_len = info[8]
    q_pos = info[qi] + lax.broadcasted_iota(jnp.int32, (1, TILE), 1)
    q_low = jnp.where(q_pos >= first_len, first_len, 0)
    k_pos = kp_ref[...] + chunk * chunk_len
    return (k_pos <= q_pos) & (k_pos >= q_low)


def self_fwd_kernel(info, q_ref, kp_ref, *refs):
    kvs, (o_ref, lse_ref, kvt, m_s, l_s, acc) = refs[:4], refs[4:]
    qi = pl.program_id(1)
    chunk_len = kvs[0].shape[0]

    @pl.when(qi == 0)
    def _():
        for back in range(4):
            kvt[back] = kvs[back][...].T

    m_s[...] = jnp.full_like(m_s, -jnp.inf)
    l_s[...] = jnp.zeros_like(l_s)
    acc[...] = jnp.zeros_like(acc)
    query = q_ref[...]

    def step(back, allowed):
        scores = nt(kvs[back][...], query)
        if allowed is not None:
            scores = jnp.where(allowed, scores, NEG_FILL)
        m_old = m_s[...]
        m_new = jnp.maximum(m_old, jnp.max(scores, axis=0, keepdims=True))
        prob = jnp.exp(scores - m_new)
        fade = jnp.exp(m_old - m_new)
        l_s[...] = l_s[...] * fade + jnp.sum(prob, axis=0, keepdims=True)
        acc[...] = acc[...] * fade + nn(kvt[back], prob.astype(BF))
        m_s[...] = m_new

    for back in range(4):
        active, masked, chunk = chunk_state(info, qi, back, chunk_len)
        if back == 0:
            step(0, self_mask(info, qi, chunk, chunk_len, kp_ref))
            continue

        @pl.when(active & jnp.logical_not(masked))
        def _(back=back):
            step(back, None)

        @pl.when(active & masked)
        def _(back=back, chunk=chunk):
            step(back, self_mask(info, qi, chunk, chunk_len, kp_ref))

    total = l_s[...]
    o_ref[...] = (acc[...] / total).T.astype(BF)
    lse_ref[0] = m_s[...] + jnp.log(total)


def self_bwd_kernel(info, q_ref, do_ref, o_ref, lse_ref, kp_ref, *refs):
    kvs, dq_ref, dkvs, (kvt, acc, dq_acc) = refs[:4], refs[4], refs[5:9], refs[9:]
    qi = pl.program_id(1)
    chunk_len = kvs[0].shape[0]

    @pl.when(qi == 0)
    def _():
        for back in range(4):
            kvt[back] = kvs[back][...].T
        acc[...] = jnp.zeros_like(acc)

    dq_acc[...] = jnp.zeros_like(dq_acc)
    query = q_ref[...]
    d_out = do_ref[...]
    lse = lse_ref[0]
    product = d_out.astype(F32) * o_ref[...].astype(F32)
    delta = jnp.sum(product.T, axis=0, keepdims=True)

    def step(back, allowed):
        scores = nt(kvs[back][...], query)
        if allowed is not None:
            scores = jnp.where(allowed, scores, NEG_FILL)
        prob = jnp.exp(scores - lse)
        d_prob = nt(kvs[back][...], d_out)
        d_score = (prob * (d_prob - delta)).astype(BF)
        acc[back] += nn(prob.astype(BF), d_out) + nn(d_score, query)
        dq_acc[...] += nn(kvt[back], d_score)

    for back in range(4):
        active, masked, chunk = chunk_state(info, qi, back, chunk_len)
        if back == 0:
            step(0, self_mask(info, qi, chunk, chunk_len, kp_ref))
            continue

        @pl.when(active & jnp.logical_not(masked))
        def _(back=back):
            step(back, None)

        @pl.when(active & masked)
        def _(back=back, chunk=chunk):
            step(back, self_mask(info, qi, chunk, chunk_len, kp_ref))

    dq_ref[...] = (dq_acc[...] * SCALING).T.astype(BF)

    @pl.when(qi == pl.num_programs(1) - 1)
    def _():
        for back in range(4):
            dkvs[back][...] = acc[back].astype(BF)


def cross_fwd_kernel(info, q_ref, kv_ref, bias_ref, o_ref, lse_ref):
    scores = nt(kv_ref[0], q_ref[...]) + bias_ref[0]
    largest = jnp.max(scores, axis=0, keepdims=True)
    prob = jnp.exp(scores - largest)
    total = jnp.sum(prob, axis=0, keepdims=True)
    out = nn(kv_ref[0].T, prob.astype(BF))
    o_ref[...] = (out / total).T.astype(BF)
    lse_ref[0] = largest + jnp.log(total)


def cross_bwd_kernel(
    info, q_ref, do_ref, o_ref, lse_ref, kv_ref, bias_ref, dq_ref, dkv_ref, acc
):
    qi = pl.program_id(1)
    side = info[qi]

    @pl.when(qi == 0)
    def _():
        acc[...] = jnp.zeros_like(acc)

    query = q_ref[...]
    d_out = do_ref[...]
    product = d_out.astype(F32) * o_ref[...].astype(F32)
    delta = jnp.sum(product.T, axis=0, keepdims=True)
    prob = jnp.exp(nt(kv_ref[0], query) + bias_ref[0] - lse_ref[0])
    d_prob = nt(kv_ref[0], d_out)
    d_score = (prob * (d_prob - delta)).astype(BF)
    acc[side] += nn(prob.astype(BF), d_out) + nn(d_score, query)
    dq_ref[...] = (nn(kv_ref[0].T, d_score) * SCALING).T.astype(BF)

    @pl.when(qi == pl.num_programs(1) - 1)
    def _():
        dkv_ref[...] = acc[...].astype(BF)


def cost(heads, rows, keys, products, moved):
    return pl.CostEstimate(
        flops=2 * products * heads * rows * keys * LANES,
        transcendentals=heads * rows * keys,
        bytes_accessed=moved,
    )


def params():
    return pltpu.CompilerParams(
        dimension_semantics=("arbitrary", "arbitrary"), vmem_limit_bytes=40 << 20
    )


def self_forward(info, queries, key_place, chunks):
    rows, width = queries.shape
    heads, steps = width // LANES, rows // TILE
    row_spec = pl.BlockSpec((TILE, LANES), lambda h, i, s: (i, h))
    head_spec = pl.BlockSpec((rows, LANES), lambda h, i, s: (0, h))
    return pl.pallas_call(
        self_fwd_kernel,
        out_shape=(
            jax.ShapeDtypeStruct((rows, width), BF),
            jax.ShapeDtypeStruct((heads, 1, rows), F32),
        ),
        grid_spec=pltpu.PrefetchScalarGridSpec(
            num_scalar_prefetch=1,
            grid=(heads, steps),
            in_specs=[row_spec, pl.BlockSpec((rows, 1), lambda h, i, s: (0, 0))]
            + [head_spec] * 4,
            out_specs=[row_spec, pl.BlockSpec((1, 1, TILE), lambda h, i, s: (h, 0, i))],
            scratch_shapes=[
                pltpu.VMEM((4, LANES, rows), BF),
                pltpu.VMEM((1, TILE), F32),
                pltpu.VMEM((1, TILE), F32),
                pltpu.VMEM((LANES, TILE), F32),
            ],
        ),
        compiler_params=params(),
        cost_estimate=cost(heads, rows, 3 * rows, 2, 6 * rows * width * 2),
    )(info, queries, key_place, *chunks)


def self_backward(info, queries, d_out, out, lse, key_place, chunks):
    rows, width = queries.shape
    heads, steps = width // LANES, rows // TILE
    row_spec = pl.BlockSpec((TILE, LANES), lambda h, i, s: (i, h))
    head_spec = pl.BlockSpec((rows, LANES), lambda h, i, s: (0, h))
    lse_spec = pl.BlockSpec((1, 1, TILE), lambda h, i, s: (h, 0, i))
    return pl.pallas_call(
        self_bwd_kernel,
        out_shape=(jax.ShapeDtypeStruct((rows, width), BF),) * 5,
        grid_spec=pltpu.PrefetchScalarGridSpec(
            num_scalar_prefetch=1,
            grid=(heads, steps),
            in_specs=[row_spec] * 3
            + [lse_spec, pl.BlockSpec((rows, 1), lambda h, i, s: (0, 0))]
            + [head_spec] * 4,
            out_specs=[row_spec] + [head_spec] * 4,
            scratch_shapes=[
                pltpu.VMEM((4, LANES, rows), BF),
                pltpu.VMEM((4, rows, LANES), F32),
                pltpu.VMEM((LANES, TILE), F32),
            ],
        ),
        compiler_params=params(),
        cost_estimate=cost(heads, rows, 3 * rows, 5, 12 * rows * width * 2),
    )(info, queries, d_out, out, lse, key_place, *chunks)


def cross_specs(rows, keys):
    row_spec = pl.BlockSpec((TILE, LANES), lambda h, i, s: (i, h))
    kv_spec = pl.BlockSpec((1, keys, LANES), lambda h, i, s: (s[i], 0, h))
    bias_spec = pl.BlockSpec((1, keys, 1), lambda h, i, s: (i % 2, 0, 0))
    lse_spec = pl.BlockSpec((1, 1, TILE), lambda h, i, s: (h, 0, i))
    return row_spec, kv_spec, bias_spec, lse_spec


def cross_forward(side, queries, pairs, bias):
    rows, width = queries.shape
    heads, steps, keys = width // LANES, rows // TILE, pairs.shape[1]
    row_spec, kv_spec, bias_spec, lse_spec = cross_specs(rows, keys)
    return pl.pallas_call(
        cross_fwd_kernel,
        out_shape=(
            jax.ShapeDtypeStruct((rows, width), BF),
            jax.ShapeDtypeStruct((heads, 1, rows), F32),
        ),
        grid_spec=pltpu.PrefetchScalarGridSpec(
            num_scalar_prefetch=1,
            grid=(heads, steps),
            in_specs=[row_spec, kv_spec, bias_spec],
            out_specs=[row_spec, lse_spec],
        ),
        compiler_params=params(),
        cost_estimate=cost(heads, rows, keys, 2, 6 * rows * width * 2),
    )(side, queries, pairs, bias)


def cross_backward(side, queries, d_out, out, lse, pairs, bias):
    rows, width = queries.shape
    heads, steps, keys = width // LANES, rows // TILE, pairs.shape[1]
    row_spec, kv_spec, bias_spec, lse_spec = cross_specs(rows, keys)
    return pl.pallas_call(
        cross_bwd_kernel,
        out_shape=(
            jax.ShapeDtypeStruct((rows, width), BF),
            jax.ShapeDtypeStruct(pairs.shape, BF),
        ),
        grid_spec=pltpu.PrefetchScalarGridSpec(
            num_scalar_prefetch=1,
            grid=(heads, steps),
            in_specs=[row_spec] * 3 + [lse_spec, kv_spec, bias_spec],
            out_specs=[row_spec, pl.BlockSpec((2, keys, LANES), lambda h, i, s: (0, 0, h))],
            scratch_shapes=[pltpu.VMEM((2, keys, LANES), F32)],
        ),
        compiler_params=params(),
        cost_estimate=cost(heads, rows, keys, 5, 12 * rows * width * 2),
    )(side, queries, d_out, out, lse, pairs, bias)


FLIPS = (0, 2, 1, 3)


def swap(array, axis, bit, size=4):
    return lax.ppermute(array, axis, [(i, i ^ bit) for i in range(size)])


def collect_rows(own):
    near = jnp.concatenate([own, swap(own, "tp", 2)], axis=0)
    return jnp.concatenate([near, swap(near, "tp", 1)], axis=0)


def spread_rows(left, right):
    half = left.shape[0] // 2
    far = nn(left[half:], right).astype(BF)
    near = nn(left[:half], right) + swap(far, "tp", 1).astype(F32)
    quarter = half // 2
    return near[:quarter] + swap(near[quarter:].astype(BF), "tp", 2).astype(F32)


def order_rows(array, tp_place):
    quarter = array.shape[0] // 4
    return jnp.concatenate(
        [
            lax.dynamic_slice_in_dim(array, (tp_place ^ flip) * quarter, quarter, 0)
            for flip in FLIPS
        ],
        axis=0,
    )


def norm_parts(residual):
    average = jnp.mean(residual, axis=-1, keepdims=True)
    centred = residual - average
    variance = jnp.mean(centred * centred, axis=-1, keepdims=True)
    inverse = lax.rsqrt(variance + 1e-05)
    return centred * inverse, inverse


def norm_back(normed, inverse, gain, upstream):
    scaled = upstream * gain
    first = jnp.mean(scaled, axis=-1, keepdims=True)
    second = jnp.mean(scaled * normed, axis=-1, keepdims=True)
    d_resid = (scaled - first - normed * second) * inverse
    return d_resid, jnp.sum(upstream * normed, axis=0), jnp.sum(upstream, axis=0)


def gelu_parts(hidden):
    cdf = 0.5 * (1.0 + lax.erf(hidden * (2.0**-0.5)))
    density = jnp.exp(-0.5 * hidden * hidden) * ((2.0 * jnp.pi) ** -0.5)
    return hidden * cdf, cdf + hidden * density


def heads_of(weight):
    return weight.reshape(weight.shape[:-1] + (-1, HEAD))


def pad_front(weight):
    split = heads_of(weight)
    return jnp.concatenate([jnp.zeros_like(split), split], axis=-1).reshape(
        weight.shape[0], -1
    )


def pad_back(weight):
    split = heads_of(weight)
    return jnp.concatenate([split, jnp.zeros_like(split)], axis=-1).reshape(
        weight.shape[0], -1
    )


def pack_pair(first, second):
    return jnp.concatenate([heads_of(first), heads_of(second)], axis=-1).reshape(
        first.shape[0], -1
    )


def lanes_of(array, place):
    split = array.reshape(array.shape[0], -1, 2, HEAD)
    return split[:, :, place].reshape(array.shape[0], -1)


def per_device(
    tokens,
    encoder_states,
    lengths,
    enc_pick,
    cotangent,
    w_self,
    w_self_out,
    w_cross,
    w_cross_out,
    w_up,
    w_down,
    b_self,
    b_cross,
    b_up,
    out_bias,
    ln_gain,
    ln_shift,
):
    def gather(shard):
        return lax.all_gather(shard, "fsdp", axis=0, tiled=True)

    self_kv = gather(pack_pair(w_self[:, 1], w_self[:, 2]))
    self_q = gather(pad_back(w_self[:, 0]))
    cross_kv = gather(pack_pair(w_cross[:, 1], w_cross[:, 2]))
    self_out = gather(pad_front(w_self_out))
    cross_q = gather(pad_back(w_cross[:, 0]))
    cross_out = gather(pad_front(w_cross_out))
    up = gather(w_up)
    down = gather(w_down)

    gains = ln_gain.astype(F32)
    shifts = ln_shift.astype(F32)
    biases = out_bias.astype(F32)
    bias_q = pad_back(b_self[:1]).astype(F32)
    bias_kv = pad_front(b_self[1:]).astype(F32)
    bias_cq = pad_back(b_cross[:1]).astype(F32)
    bias_ckv = pad_front(b_cross[1:]).astype(F32)
    bias_up = b_up.astype(F32)

    micro = tokens.shape[0]
    tok_count = tokens.shape[1]
    quarter = tok_count // 4
    enc_count = encoder_states.shape[1]
    ctx_place = lax.axis_index("ctx")
    tp_place = lax.axis_index("tp")
    odd = ctx_place % 2 == 1
    flips = jnp.array(FLIPS, jnp.int32)
    places = tp_place ^ flips
    in_chunk = (places[:, None] * quarter + jnp.arange(quarter, dtype=jnp.int32)).reshape(-1)
    key_place = in_chunk[:, None]
    block_start = ctx_place * tok_count + (places // 2) * QBLK
    own_base = jnp.where(odd, enc_count, 0)
    far_base = jnp.where(ctx_place == 1, 0, enc_count)
    pair_places = jnp.stack(
        [
            jnp.concatenate([in_chunk + own_base, in_chunk + enc_count - own_base]),
            jnp.concatenate([in_chunk + far_base, in_chunk + enc_count - far_base]),
        ]
    )
    chain = [(i, i + 1) for i in range(3)]
    back = [(i + 1, i) for i in range(3)]

    def send(array, pairs):
        return lax.ppermute(array, "ctx", pairs)

    M = range(micro)
    x = [order_rows(tokens[m], tp_place) for m in M]
    enc = [order_rows(encoder_states[m], tp_place) for m in M]
    x_own = [x[m][:quarter].astype(F32) for m in M]

    chunks, queries, self_info, pairs = [], [], [], []
    for m in M:
        own = (nn(x[m], self_kv) + bias_kv).astype(BF)
        one = send(own, chain)
        two = send(one, chain[1:])
        three = send(two, chain[2:])
        chunks.append((own, one, two, three))
        queries.append(((nn(x[m], self_q) + bias_q) * SCALING).astype(BF))
        first_len = lengths[m, 0, 0]
        self_info.append(
            jnp.concatenate(
                [
                    ctx_place * tok_count + places * quarter,
                    jnp.zeros((4,), jnp.int32),
                    jnp.stack([first_len, ctx_place]),
                ]
            )
        )
    side, key_bias = [], []
    for m in M:
        own = (nn(enc[m], cross_kv) + bias_ckv).astype(BF)
        rise = send(own, chain)
        fall = send(own, back)
        rise_far = send(rise, chain[1:2])
        fall_far = send(fall, back[1:2])
        pairs.append(
            jnp.stack(
                [
                    jnp.concatenate([own, jnp.where(odd, rise, fall)]),
                    jnp.concatenate(
                        [
                            jnp.where(odd, fall, rise),
                            jnp.where(ctx_place == 1, fall_far, rise_far),
                        ]
                    ),
                ]
            )
        )
        second = (block_start >= lengths[m, 0, 0]).astype(jnp.int32)
        chosen = (second != ctx_place // 2).astype(jnp.int32)
        side.append(chosen)
        fills = []
        for i in range(2):
            picks = lax.dynamic_index_in_dim(enc_pick[m], places[i] // 2, 0, keepdims=False)
            spots = lax.dynamic_index_in_dim(pair_places, chosen[i], 0, keepdims=False)
            hit = jnp.any(spots[:, None] == picks[None, :], axis=1)
            fills.append(jnp.where(hit, 0.0, NEG_FILL))
        key_bias.append(jnp.stack(fills)[:, :, None])

    attended, self_lse, first, first_n, first_inv = [], [], [], [], []
    first_own = []
    for m in M:
        out, lse = self_forward(self_info[m], queries[m], key_place, chunks[m])
        attended.append(out)
        self_lse.append(lse)
        resid = x_own[m] + spread_rows(out, self_out.T) + biases[0]
        normed, inverse = norm_parts(resid)
        first_n.append(normed)
        first_inv.append(inverse)
        own = (normed * gains[0] + shifts[0]).astype(BF)
        first_own.append(own)
        first.append(collect_rows(own))

    cross_query, cross_att, cross_lse, second, second_n, second_inv, second_own = (
        [] for _ in range(7)
    )
    for m in M:
        query = ((nn(first[m], cross_q) + bias_cq) * SCALING).astype(BF)
        cross_query.append(query)
        out, lse = cross_forward(side[m], query, pairs[m], key_bias[m])
        cross_att.append(out)
        cross_lse.append(lse)
        resid = first_own[m].astype(F32) + spread_rows(out, cross_out.T) + biases[1]
        normed, inverse = norm_parts(resid)
        second_n.append(normed)
        second_inv.append(inverse)
        own = (normed * gains[1] + shifts[1]).astype(BF)
        second_own.append(own)
        second.append(collect_rows(own))

    outputs, active, slope, d_third, d_ffn, sums = [], [], [], [], [], []
    small = []
    for m in M:
        value, grade = gelu_parts(nn(second[m], up) + bias_up)
        active.append(value.astype(BF))
        slope.append(grade.astype(BF))
        resid = second_own[m].astype(F32) + spread_rows(active[m], down.T) + biases[2]
        normed, inverse = norm_parts(resid)
        outputs.append(normed * gains[2] + shifts[2])
        d_resid, d_gain, d_shift = norm_back(
            normed, inverse, gains[2], cotangent[m].astype(F32)
        )
        d_third.append(d_resid)
        small.append([d_gain, d_shift, jnp.sum(d_resid, axis=0)])
        d_ffn.append(collect_rows(d_resid.astype(BF)))

    d_hidden, d_second_res, d_cross = [], [], []
    for m in M:
        grad = (nn(d_ffn[m], down) * slope[m].astype(F32)).astype(BF)
        d_hidden.append(grad)
        upstream = d_third[m] + spread_rows(grad, up.T)
        d_resid, d_gain, d_shift = norm_back(second_n[m], second_inv[m], gains[1], upstream)
        d_second_res.append(d_resid)
        small[m] += [d_gain, d_shift, jnp.sum(d_resid, axis=0)]
        d_cross.append(collect_rows(d_resid.astype(BF)))

    def total(lefts, rights):
        return functools.reduce(jnp.add, [tn(a, b) for a, b in zip(lefts, rights)])

    def scatter(grad):
        part = lax.psum_scatter(grad.astype(BF), "fsdp", scatter_dimension=0, tiled=True)
        return lax.psum(part, "ctx").astype(F32)

    grad_up = scatter(total(second, d_hidden))
    grad_down = scatter(total(d_ffn, active))

    d_cross_query, d_pairs, d_first_res, d_self, grad_encoders = [], [], [], [], []
    d_enc_pairs = []
    for m in M:
        d_att = nn(d_cross[m], cross_out).astype(BF)
        d_query, d_pair = cross_backward(
            side[m], cross_query[m], d_att, cross_att[m], cross_lse[m], pairs[m], key_bias[m]
        )
        d_cross_query.append(d_query)
        own, near = d_pair[0, :enc_count], d_pair[0, enc_count:].astype(F32)
        other, far = d_pair[1, :enc_count], d_pair[1, enc_count:]
        gained = send(far, chain[1:2] + back[1:2])
        near = (near + gained.astype(F32)).astype(BF)
        rise = send(jnp.where(odd, other, near), chain)
        fall = send(jnp.where(odd, near, other), back)
        d_enc = (own.astype(F32) + rise.astype(F32) + fall.astype(F32)).astype(BF)
        d_enc_pairs.append(d_enc)
        upstream = d_second_res[m] + spread_rows(d_query, cross_q.T)
        d_resid, d_gain, d_shift = norm_back(first_n[m], first_inv[m], gains[0], upstream)
        d_first_res.append(d_resid)
        small[m] += [d_gain, d_shift, jnp.sum(d_resid, axis=0)]
        d_self.append(collect_rows(d_resid.astype(BF)))
    for m in M:
        grad_encoders.append(spread_rows(d_enc_pairs[m], cross_kv.T))

    width = w_self_out.shape[1]
    grad_cross_out = lanes_of(total(d_cross, cross_att), 1)
    grad_cross_q = lanes_of(total(first, d_cross_query), 0)
    grad_cross_kv = total(enc, d_enc_pairs)
    packed = scatter(
        jnp.concatenate(
            [
                grad_cross_out,
                grad_cross_q,
                lanes_of(grad_cross_kv, 0),
                lanes_of(grad_cross_kv, 1),
            ],
            axis=1,
        )
    )
    grad_cross_out = packed[:, :width]
    grad_cross = packed[:, width:].reshape(packed.shape[0], 3, width)

    d_queries, d_own, grad_inputs = [], [], []
    for m in M:
        d_att = nn(d_self[m], self_out).astype(BF)
        d_query, *d_chunks = self_backward(
            self_info[m], queries[m], d_att, attended[m], self_lse[m], key_place, chunks[m]
        )
        d_queries.append(d_query)
        moving = send(d_chunks[3], back[2:])
        moving = (d_chunks[2].astype(F32) + moving.astype(F32)).astype(BF)
        moving = send(moving, back[1:])
        moving = (d_chunks[1].astype(F32) + moving.astype(F32)).astype(BF)
        moving = send(moving, back)
        d_own.append((d_chunks[0].astype(F32) + moving.astype(F32)).astype(BF))
    both = jnp.concatenate([self_q, self_kv], axis=1).T
    for m in M:
        joined = jnp.concatenate([d_queries[m], d_own[m]], axis=1)
        grad_inputs.append(d_first_res[m] + spread_rows(joined, both))

    grad_self_out = lanes_of(total(d_self, attended), 1)
    grad_self_q = lanes_of(total(x, d_queries), 0)
    grad_self_kv = total(x, d_own)
    packed = scatter(
        jnp.concatenate(
            [
                grad_self_out,
                grad_self_q,
                lanes_of(grad_self_kv, 0),
                lanes_of(grad_self_kv, 1),
            ],
            axis=1,
        )
    )
    grad_self_out = packed[:, :width]
    grad_self = packed[:, width:].reshape(packed.shape[0], 3, width)

    def row_sum(arrays):
        return functools.reduce(
            jnp.add, [jnp.sum(a.astype(F32), axis=0, keepdims=True) for a in arrays]
        )

    local = jnp.concatenate(
        [
            lanes_of(row_sum(d_queries), 0),
            lanes_of(row_sum(d_own), 1),
            lanes_of(row_sum(d_cross_query), 0),
            lanes_of(row_sum(d_enc_pairs), 1),
            row_sum(d_hidden),
        ],
        axis=1,
    )[0]
    common = functools.reduce(jnp.add, [jnp.concatenate(small[m]) for m in M])
    for bit in (1, 2):
        common = common + swap(common, "tp", bit)
    count = local.shape[0]
    joined = jnp.concatenate([local, common])
    for bit in (1, 2):
        joined = joined + swap(joined, "ctx", bit)
    fsdp = lax.axis_size("fsdp")
    bit = 1
    while bit < fsdp:
        joined = joined + swap(joined, "fsdp", bit, fsdp)
        bit *= 2
    local, common = joined[:count], joined[count:].reshape(3, 3, -1)
    return (
        jnp.stack(outputs),
        jnp.stack(grad_inputs),
        jnp.stack(grad_encoders),
        grad_self,
        grad_self_out,
        grad_cross,
        grad_cross_out,
        grad_up,
        grad_down,
        local[: 2 * width].reshape(2, width),
        local[2 * width : 4 * width].reshape(2, width),
        local[4 * width :],
        common[::-1, 2],
        common[::-1, 0],
        common[::-1, 1],
    )


def solution(mesh):
    return jax.shard_map(
        per_device,
        mesh=mesh,
        in_specs=(
            P(None, ("fsdp", "ctx"), None),
            P(None, ("fsdp", "ctx"), None),
            P(None, "fsdp", None),
            P(None, ("fsdp", "ctx"), None),
            P(None, ("fsdp", "ctx", "tp"), None),
            P("fsdp", None, "tp"),
            P("fsdp", "tp"),
            P("fsdp", None, "tp"),
            P("fsdp", "tp"),
            P("fsdp", "tp"),
            P("fsdp", "tp"),
            P(None, "tp"),
            P(None, "tp"),
            P("tp"),
            P(),
            P(),
            P(),
        ),
        out_specs=(
            P(None, ("fsdp", "ctx", "tp"), None),
            P(None, ("fsdp", "ctx", "tp"), None),
            P(None, ("fsdp", "ctx", "tp"), None),
            P("fsdp", None, "tp"),
            P("fsdp", "tp"),
            P("fsdp", None, "tp"),
            P("fsdp", "tp"),
            P("fsdp", "tp"),
            P("fsdp", "tp"),
            P(None, "tp"),
            P(None, "tp"),
            P("tp"),
            P(),
            P(),
            P(),
        ),
        check_vma=False,
    )
```
